32 devices in a mesh: dp: 16 (over z, y, core), mp: 2 (over x).
Axes of the slice: x: 2, y: 2, z: 4, core: 2. Of those that a mesh axis runs over, the one named last changes fastest.
Arguments:
- picture_tower_vectors: bfloat16 [3072, 1152], P('dp'), may hold values from -6 to 6
- caption_tower_vectors: bfloat16 [3072, 1152], P('dp', 'mp'), may hold values from -6 to 6
- picture_standardize_factor: float32 [1152], replicated, may hold values from 0.1 to 1.9
- picture_entry_matrix: bfloat16 [1152, 4304], P(None, 'mp'), may hold values from -0.1875 to 0.1875
- picture_exit_matrix: bfloat16 [4304, 1152], P('mp'), may hold values from -0.09375 to 0.09375
- caption_mapping_matrix: bfloat16 [1152, 1152], P('mp'), may hold values from -1 to 1
- energy_multiplier: float32 [], replicated, may hold values from 4 to 16
- energy_offset_term: float32 [], replicated, may hold values from -2 to -0.5
Outputs:
- grad_image: float32 [3072, 1152], P('dp', 'mp')
- grad_text: float32 [3072, 1152], P('dp', 'mp')
The draws below stay inside these ranges and needn't reach their ends.
All inputs are finite; a program needn't handle non-finite values.
Results may differ from the reference program's by a relative error of at most 0.0046.
Values may be sent and summed in bfloat16 or wider, within the bound.
A program may use at most 64 MiB of HBM per device.

```python
import math
import jax
import jax.numpy as jnp
from jax import lax

D = 1152
FF = 4304
ROWS = 192
PAIRS = 3072
N_DP = 16


def cluster_centres(key):
    anchor_rows = jax.random.normal(jax.random.fold_in(key, 101), (8, D), jnp.float32)
    prototypes = jnp.concatenate([anchor_rows, -anchor_rows], axis=0)
    labels = jax.random.randint(jax.random.fold_in(key, 102), (PAIRS,), 0, 16)
    return prototypes[labels]


def mapping_weights(key):
    entries = jax.random.normal(jax.random.fold_in(key, 103), (D, D), jnp.float32)
    return jnp.clip(entries * (1.0 / math.sqrt(D)), -1.0, 1.0)


def jitter_rows(key):
    return jax.random.normal(key, (PAIRS, D), jnp.float32)


def mix_weights():
    return (0.8, 0.6)


def draw_picture_tower_vectors(key, part):
    centres = cluster_centres(key)
    cluster_weight, jitter_weight = mix_weights()
    values = cluster_weight * centres + jitter_weight * jitter_rows(jax.random.fold_in(key, 104))
    return jnp.clip(values, -6.0, 6.0).astype(jnp.bfloat16)


def draw_caption_tower_vectors(key, part):
    centres = cluster_centres(key)
    mapped = lax.dot_general(centres, mapping_weights(key), (((1,), (1,)), ((), ())), precision=lax.Precision.HIGHEST)
    cluster_weight, jitter_weight = mix_weights()
    values = cluster_weight * mapped + jitter_weight * jitter_rows(jax.random.fold_in(key, 105))
    return jnp.clip(values, -6.0, 6.0).astype(jnp.bfloat16)


def draw_caption_mapping_matrix(key, part):
    return mapping_weights(key).astype(jnp.bfloat16)


def shard_levels(rng, dims, cuts, low, largest):
    level = 1.0
    for axis_at, shards_of in cuts:
        steps = jax.random.uniform(jax.random.fold_in(jax.random.fold_in(rng, 6), axis_at), (shards_of,), jnp.float32, low / len(cuts), largest / len(cuts))
        level = level * jnp.repeat(jnp.exp(steps), dims[axis_at] // shards_of).reshape((-1,) + (1,) * (len(dims) - 1 - axis_at))
    return level


def gaussian(own_key, extent, scale, most, pieces=(), kind=jnp.bfloat16):
    level = shard_levels(own_key, extent, pieces, -0.22, 0.18) if pieces else 1.0
    result = jax.random.normal(own_key, extent, jnp.float32) * scale * level
    return jnp.minimum(jnp.maximum(result, -most), most).astype(kind)


def setup_inputs(seed: int = 0) -> dict:
    arg_keys = jax.random.split(jax.random.key(seed), 9)
    return {
        "picture_tower_vectors": draw_picture_tower_vectors(jax.random.fold_in(arg_keys[8], 71), 0),
        "caption_tower_vectors": draw_caption_tower_vectors(jax.random.fold_in(arg_keys[8], 71), 0),
        "picture_standardize_factor": jnp.clip(1.0 + 0.18 * jax.random.normal(arg_keys[2], (D,), jnp.float32), 0.1, 1.9),
        "picture_entry_matrix": gaussian(arg_keys[3], (D, FF), D ** -0.5, 0.1875, ((1, 2),)),
        "picture_exit_matrix": gaussian(arg_keys[4], (FF, D), FF ** -0.5, 0.09375, ((0, 2),)),
        "caption_mapping_matrix": draw_caption_mapping_matrix(jax.random.fold_in(arg_keys[8], 71), 0),
        "energy_multiplier": jnp.clip(jnp.exp(jax.random.uniform(arg_keys[6], (), jnp.float32, math.log(4.0), math.log(16.0))), 4.0, 16.0),
        "energy_offset_term": jnp.clip(jax.random.uniform(arg_keys[7], (), jnp.float32, -2.0, -0.5), -2.0, -0.5),
    }


def gelu_tanh(values):
    return jax.nn.gelu(values, approximate=True)

def norm_back(upstream, unit_rows, inverse):
    unit_float = unit_rows.astype(jnp.float32)
    along = lax.optimization_barrier(jnp.sum(unit_float * upstream, axis=-1, keepdims=True))
    return inverse * (upstream - unit_float * along)

def reference(picture_tower_vectors, caption_tower_vectors, picture_standardize_factor, picture_entry_matrix, picture_exit_matrix, caption_mapping_matrix, energy_multiplier, energy_offset_term):
    image_float = picture_tower_vectors.astype(jnp.float32)
    mean_row = lax.optimization_barrier(jnp.mean(image_float, axis=-1, keepdims=True))
    variance = lax.optimization_barrier(jnp.mean((image_float - mean_row) ** 2, axis=-1, keepdims=True))
    inv_std = lax.rsqrt(variance + 1e-06)
    centred = (image_float - mean_row) * inv_std
    normed = (centred * picture_standardize_factor).astype(jnp.bfloat16)
    preact = jnp.dot(normed, picture_entry_matrix, preferred_element_type=jnp.float32)
    hidden = gelu_tanh(preact).astype(jnp.bfloat16)
    image_out = image_float + jnp.dot(hidden, picture_exit_matrix, preferred_element_type=jnp.float32)
    inv_image = lax.rsqrt(lax.optimization_barrier(jnp.sum(image_out * image_out, axis=-1, keepdims=True)) + 1e-06)
    unit_image = (image_out * inv_image).astype(jnp.bfloat16)
    text_out = jnp.dot(caption_tower_vectors, caption_mapping_matrix, preferred_element_type=jnp.float32)
    inv_text = lax.rsqrt(lax.optimization_barrier(jnp.sum(text_out * text_out, axis=-1, keepdims=True)) + 1e-06)
    unit_text = (text_out * inv_text).astype(jnp.bfloat16)
    total = ROWS * N_DP
    image_ids = jnp.arange(total, dtype=jnp.int32)

    def block_step(image_dir, block_index):
        first = (block_index * ROWS).astype(jnp.int32)
        block_now = lax.dynamic_slice_in_dim(unit_text, first, ROWS, 0)
        text_ids = first + jnp.arange(ROWS, dtype=jnp.int32)
        cosine_matrix = lax.dot_general(block_now, unit_image, (((1,), (1,)), ((), ())), preferred_element_type=jnp.float32)
        couple_energies = energy_multiplier * cosine_matrix + energy_offset_term
        match_polarity = jnp.where(text_ids[:, None] == image_ids[None, :], 1.0, -1.0).astype(jnp.float32)
        polarity_scaled_energies = (energy_multiplier * -match_polarity * jax.nn.sigmoid(-match_polarity * couple_energies)).astype(jnp.bfloat16)
        image_dir = image_dir + lax.dot_general(polarity_scaled_energies, block_now, (((0,), (0,)), ((), ())), preferred_element_type=jnp.float32)
        text_part = jnp.dot(polarity_scaled_energies, unit_image, preferred_element_type=jnp.float32)
        return (image_dir, text_part)
    image_dir, text_parts = lax.scan(block_step, jnp.zeros((total, D), jnp.float32), jnp.arange(N_DP, dtype=jnp.int32))
    text_dir = text_parts.reshape(total, D)
    grad_out = norm_back(image_dir, unit_image, inv_image)
    grad_out_b = grad_out.astype(jnp.bfloat16)
    grad_hidden = lax.dot_general(grad_out_b, picture_exit_matrix, (((1,), (1,)), ((), ())), preferred_element_type=jnp.float32)
    unused, pull_back = jax.vjp(gelu_tanh, preact)
    grad_pre = pull_back(grad_hidden)[0].astype(jnp.bfloat16)
    grad_normed = lax.dot_general(grad_pre, picture_entry_matrix, (((1,), (1,)), ((), ())), preferred_element_type=jnp.float32)
    scaled = grad_normed * picture_standardize_factor
    mean_one = lax.optimization_barrier(jnp.mean(scaled, axis=-1, keepdims=True))
    mean_two = lax.optimization_barrier(jnp.mean(scaled * centred, axis=-1, keepdims=True))
    grad_image = grad_out + inv_std * (scaled - mean_one - centred * mean_two)
    grad_text_out = norm_back(text_dir, unit_text, inv_text).astype(jnp.bfloat16)
    grad_text = lax.dot_general(grad_text_out, caption_mapping_matrix, (((1,), (1,)), ((), ())), preferred_element_type=jnp.float32)
    return (grad_image, grad_text)
```

```python
import functools
import math

import jax
import jax.numpy as jnp
from jax import lax
from jax.experimental import pallas as pl
from jax.experimental.pallas import tpu as pltpu
from jax.sharding import PartitionSpec as P

F32 = jnp.float32
BF16 = jnp.bfloat16
MESH = pl.DeviceIdType.MESH
TILE = 512
ROOT = math.sqrt(2.0 / math.pi)
NT = (((1,), (1,)), ((), ()))


def dot(a, b):
    return jnp.dot(a, b, preferred_element_type=F32)


def dot_nt(a, b):
    return lax.dot_general(a, b, NT, preferred_element_type=F32)


def gelu_pair(x):
    square = x * x
    t = jnp.tanh(ROOT * (x + 0.044715 * (square * x)))
    half = 0.5 * (1.0 + t)
    slope = half + 0.5 * x * (1.0 - t * t) * (ROOT * (1.0 + 0.134145 * square))
    return x * half, slope


def norm_back(upstream, unit_rows, inverse):
    unit_float = unit_rows.astype(F32)
    along = jnp.sum(unit_float * upstream, axis=-1, keepdims=True)
    return inverse * (upstream - unit_float * along)


def body(
    n,
    heads,
    pic_hbm,
    split_hbm,
    cap_hbm,
    gain_ref,
    gains_ref,
    entry_hbm,
    exit_hbm,
    map_hbm,
    scale_ref,
    shift_ref,
    out_go,
    out_rest,
    out_text,
    pic,
    split,
    cap,
    entry,
    exit_,
    mapping,
    load_sem,
    normed,
    slope,
    acc,
    own_f32,
    parts,
    lands,
    fulls,
    ring_text,
    ring_image,
    norm_own,
    norm_part,
    norm_land,
    sums_part,
    sums_land,
    part_send,
    part_recv,
    full_send,
    full_recv,
    norm_send,
    norm_recv,
    sums_send,
    sums_recv,
    ring_send,
    ring_recv,
):
    rows, width = pic.shape
    share = rows // heads
    hidden = entry.shape[1]
    cols = split.shape[2]
    me = lax.axis_index("dp")
    head = lax.axis_index("mp")
    length = n // 4

    def place(index):
        z = index // 4
        y = (index // 2) % 2
        return 2 * (z * (1 - y) + (2 * length - 1 - z) * y) + index % 2

    def device(position):
        position = (position + n) % n
        chip = position // 2
        y = chip // length
        z = chip * (1 - y) + (2 * length - 1 - chip) * y
        return (z * 2 + y) * 2 + position % 2

    pos = place(me)
    right = device(pos + 1)
    left = device(pos - 1)
    forward = n // 2
    backward = n - 1 - forward

    loads = []
    for at, (src, dst) in enumerate(
        (
            (cap_hbm, cap),
            (map_hbm, mapping),
            (pic_hbm, pic),
            (entry_hbm, entry),
            (exit_hbm, exit_),
            (split_hbm, split),
        )
    ):
        copy = pltpu.make_async_copy(src, dst, load_sem.at[at])
        copy.start()
        loads.append(copy)

    barrier = pltpu.get_barrier_semaphore()
    for neighbour in (left, right):
        pl.semaphore_signal(barrier, inc=1, device_id={"dp": neighbour}, device_id_type=MESH)
    for o in range(1, heads):
        pl.semaphore_signal(
            barrier, inc=1, device_id={"mp": (head + o) % heads}, device_id_type=MESH
        )

    def ring_copy(which, buf, way, step):
        block = device(pos - step if way == 0 else pos + step)
        return pltpu.make_async_remote_copy(
            src_ref=buf.at[block],
            dst_ref=buf.at[block],
            send_sem=ring_send.at[which, way, step],
            recv_sem=ring_recv.at[which, way, step],
            device_id={"dp": right if way == 0 else left},
            device_id_type=MESH,
        )

    def ring_start(which, buf, step):
        if step < forward:
            ring_copy(which, buf, 0, step).start()
        if step < backward:
            ring_copy(which, buf, 1, step).start()

    def ring_next(which, buf, step):
        for way, count in ((0, forward), (1, backward)):
            if step < count:
                block = device(pos - step - 1 if way == 0 else pos + step + 1)
                pltpu.make_async_remote_copy(
                    src_ref=buf.at[block],
                    dst_ref=buf.at[block],
                    send_sem=ring_send.at[which, way, step],
                    recv_sem=ring_recv.at[which, way, step],
                    device_id={"dp": right if way == 0 else left},
                    device_id_type=MESH,
                ).wait_recv()
                if step + 1 < count:
                    ring_copy(which, buf, way, step + 1).start()

    def ring_end(which, buf):
        for way, count in ((0, forward), (1, backward)):
            for step in range(count):
                ring_copy(which, buf, way, step).wait_send()

    def exchange(src, dst, send, recv, spread):
        copies = []
        for o in range(1, heads):
            to = (head + o) % heads
            source = (head + heads - o) % heads
            sent = pltpu.make_async_remote_copy(
                src_ref=src.at[to] if spread else src.at[head],
                dst_ref=dst.at[head],
                send_sem=send.at[o],
                recv_sem=recv.at[o],
                device_id={"mp": to},
                device_id_type=MESH,
            )
            got = pltpu.make_async_remote_copy(
                src_ref=dst.at[source],
                dst_ref=dst.at[source],
                send_sem=send.at[o],
                recv_sem=recv.at[o],
                device_id={"mp": to},
                device_id_type=MESH,
            )
            copies.append((sent, got))
        for sent, got in copies:
            sent.start()
        return copies

    def arrived(copies):
        for sent, got in copies:
            got.wait_recv()

    def finished(copies):
        for sent, got in copies:
            sent.wait_send()

    def scatter_start(which, total):
        for p in range(heads):
            piece = total[p * share : (p + 1) * share]
            own_f32[p] = piece
            parts[which, p] = piece.astype(BF16)
        return exchange(
            parts.at[which], lands.at[which], part_send.at[which], part_recv.at[which], True
        )

    def scatter_sum(which, copies, mine):
        arrived(copies)
        for o in range(1, heads):
            mine = mine + lands[which, (head + heads - o) % heads].astype(F32)
        return mine

    def share_start(which, mine):
        fulls[which, head] = mine
        return exchange(
            fulls.at[which], fulls.at[which], full_send.at[which], full_recv.at[which], False
        )

    def full(which):
        return jnp.concatenate([fulls[which, p] for p in range(heads)], axis=0)

    pending = []

    loads[0].wait()
    loads[1].wait()
    text_part = dot(cap[...], mapping[...])
    pl.semaphore_wait(barrier, 2 + heads - 1)
    text_copies = scatter_start(0, text_part)
    pending.append(text_copies)
    text_mine = own_f32[head]

    loads[2].wait()
    image_float = pic[...].astype(F32)
    mean_row = jnp.mean(image_float, axis=-1, keepdims=True)
    variance = jnp.mean((image_float - mean_row) ** 2, axis=-1, keepdims=True)
    inv_std = lax.rsqrt(variance + 1e-06)
    normed[...] = ((image_float - mean_row) * inv_std * gain_ref[...]).astype(BF16)

    text_out = scatter_sum(0, text_copies, text_mine)
    inv_text = lax.rsqrt(jnp.sum(text_out * text_out, axis=-1, keepdims=True) + 1e-06)
    unit_text = (text_out * inv_text).astype(BF16)
    ring_text[me] = unit_text
    ring_start(0, ring_text, 0)
    text_full = share_start(0, unit_text)
    pending.append(text_full)

    loads[3].wait()
    loads[4].wait()
    tiles = [(first, min(TILE, hidden - first)) for first in range(0, hidden, TILE)]
    text_steps = iter(range(forward))

    def advance(steps, which, buf, count):
        for _ in range(count):
            step = next(steps, None)
            if step is not None:
                ring_next(which, buf, step)

    for at, (first, size) in enumerate(tiles):
        span = slice(first, first + size)
        value, grad = gelu_pair(dot(normed[...], entry[:, span]))
        slope[:, span] = grad
        product = dot(value.astype(BF16), exit_[span, :])
        if at == 0:
            acc[...] = product
        else:
            acc[...] += product
        advance(text_steps, 0, ring_text, 1)
    image_copies = scatter_start(1, acc[...])
    pending.append(image_copies)
    mine = own_f32[head] + pic[pl.ds(pl.multiple_of(head * share, 8), share), :].astype(F32)
    advance(text_steps, 0, ring_text, 1)
    image_out = scatter_sum(1, image_copies, mine)
    inv_image = lax.rsqrt(jnp.sum(image_out * image_out, axis=-1, keepdims=True) + 1e-06)
    unit_image = (image_out * inv_image).astype(BF16)
    ring_image[me] = unit_image
    image_full = share_start(1, unit_image)
    pending.append(image_full)
    ring_start(1, ring_image, 0)
    advance(text_steps, 0, ring_text, forward)
    ring_end(0, ring_text)
    arrived(image_full)
    arrived(text_full)

    scale = scale_ref[0, 0]
    shift = shift_ref[0, 0]
    group = 4 if share % 16 == 0 else 1

    def terms(rows_ref, buf):
        acc[...] = jnp.zeros_like(acc)

        def one(g, carry):
            mine = full(rows_ref)
            if group == 1:
                block = buf[g]
            else:
                block = buf[pl.ds(g * group, group)].reshape(group * share, width)
            energy = scale * dot_nt(mine, block) + shift
            shape = (rows, group * share)
            column = lax.broadcasted_iota(jnp.int32, shape, 1)
            ident = column + (g * (group * rows) + head * share)
            for j in range(1, group):
                ident = ident + jnp.where(column >= j * share, rows - share, 0)
            same = ident == lax.broadcasted_iota(jnp.int32, shape, 0) + me * rows
            weight = scale * jax.nn.sigmoid(jnp.where(same, -energy, energy))
            weight = jnp.where(same, -weight, weight).astype(BF16)
            acc[...] += dot(weight, block)
            return carry

        lax.fori_loop(0, n // group, one, 0)

    image_steps = iter(range(forward))
    terms(1, ring_text)
    dir_copies = scatter_start(2, acc[...])
    pending.append(dir_copies)
    dir_mine = own_f32[head]
    advance(image_steps, 1, ring_image, 2)
    image_dir = scatter_sum(2, dir_copies, dir_mine)
    grad_out = norm_back(image_dir, fulls[1, head], inv_image)
    grad_full = share_start(2, grad_out.astype(BF16))
    pending.append(grad_full)
    advance(image_steps, 1, ring_image, 2)
    arrived(grad_full)
    for p in range(heads):
        out_go[p * share : (p + 1) * share] = fulls[2, p]

    grad_b = full(2)
    for at, (first, size) in enumerate(tiles):
        span = slice(first, first + size)
        grad_pre = (dot_nt(grad_b, exit_[span, :]) * slope[:, span]).astype(BF16)
        for p in range(heads):
            product = dot_nt(grad_pre, entry[p * cols : (p + 1) * cols, span])
            if at == 0:
                norm_own[p] = product
            else:
                norm_own[p] += product
        advance(image_steps, 1, ring_image, 1)
    loads[5].wait()
    one_sum = jnp.zeros((rows, 1), F32)
    two_sum = jnp.zeros((rows, 1), F32)
    for p in range(heads):
        piece = norm_own[p]
        norm_part[p] = piece.astype(BF16)
        scaled = piece * gains_ref[p]
        one_sum += jnp.sum(scaled, axis=-1, keepdims=True)
        centred = (split[p].astype(F32) - mean_row) * inv_std
        two_sum += jnp.sum(scaled * centred, axis=-1, keepdims=True)
    lane = lax.broadcasted_iota(jnp.int32, (rows, 128), 1)
    sums_part[head] = jnp.where(lane == 0, one_sum, two_sum)
    norm_copies = exchange(norm_part, norm_land, norm_send, norm_recv, True)
    sums_copies = exchange(sums_part, sums_land, sums_send, sums_recv, False)
    pending.append(norm_copies)
    pending.append(sums_copies)
    advance(image_steps, 1, ring_image, forward)
    ring_end(1, ring_image)

    terms(0, ring_image)
    dirs_copies = scatter_start(3, acc[...])
    pending.append(dirs_copies)
    dirs_mine = own_f32[head]

    arrived(norm_copies)
    arrived(sums_copies)
    grad_normed = norm_own[head]
    sums = sums_part[head]
    for o in range(1, heads):
        source = (head + heads - o) % heads
        grad_normed = grad_normed + norm_land[source].astype(F32)
        sums = sums + sums_land[source]
    mean_one = sums[:, 0:1] * (1.0 / width)
    mean_two = sums[:, 1:2] * (1.0 / width)
    centred = (split[head].astype(F32) - mean_row) * inv_std
    scaled = grad_normed * gains_ref[head]
    out_rest[...] = inv_std * (scaled - mean_one - centred * mean_two)

    text_dir = scatter_sum(3, dirs_copies, dirs_mine)
    grad_text_out = norm_back(text_dir, fulls[0, head], inv_text).astype(BF16)
    last_full = share_start(3, grad_text_out)
    pending.append(last_full)
    arrived(last_full)
    out_text[...] = dot_nt(full(3), mapping[...])
    for copies in pending:
        finished(copies)


def per_device(pic, cap, gain, entry, exit_, mapping, scale, shift):
    rows, width = pic.shape
    n = lax.axis_size("dp")
    heads = lax.axis_size("mp")
    cols = cap.shape[1]
    share = rows // heads
    hidden = entry.shape[1]
    split = pic.reshape(rows, heads, cols).transpose(1, 0, 2)
    anywhere = pl.BlockSpec(memory_space=pl.ANY)
    vmem = pl.BlockSpec(memory_space=pltpu.VMEM)
    smem = pl.BlockSpec(memory_space=pltpu.SMEM)
    dma = pltpu.SemaphoreType.DMA
    go, rest, text = pl.pallas_call(
        functools.partial(body, n, heads),
        out_shape=(
            jax.ShapeDtypeStruct((rows, width), BF16),
            jax.ShapeDtypeStruct((rows, cols), F32),
            jax.ShapeDtypeStruct((rows, mapping.shape[0]), F32),
        ),
        in_specs=[anywhere, anywhere, anywhere, vmem, vmem, anywhere, anywhere, anywhere, smem, smem],
        out_specs=(vmem, vmem, vmem),
        scratch_shapes=[
            pltpu.VMEM(pic.shape, BF16),
            pltpu.VMEM(split.shape, BF16),
            pltpu.VMEM(cap.shape, BF16),
            pltpu.VMEM(entry.shape, BF16),
            pltpu.VMEM(exit_.shape, BF16),
            pltpu.VMEM(mapping.shape, BF16),
            dma((6,)),
            pltpu.VMEM((rows, width), BF16),
            pltpu.VMEM((rows, hidden), F32),
            pltpu.VMEM((rows, width), F32),
            pltpu.VMEM((heads, share, width), F32),
            pltpu.VMEM((4, heads, share, width), BF16),
            pltpu.VMEM((4, heads, share, width), BF16),
            pltpu.VMEM((4, heads, share, width), BF16),
            pltpu.VMEM((n, share, width), BF16),
            pltpu.VMEM((n, share, width), BF16),
            pltpu.VMEM((heads, rows, cols), F32),
            pltpu.VMEM((heads, rows, cols), BF16),
            pltpu.VMEM((heads, rows, cols), BF16),
            pltpu.VMEM((heads, rows, 128), F32),
            pltpu.VMEM((heads, rows, 128), F32),
            dma((4, heads)),
            dma((4, heads)),
            dma((4, heads)),
            dma((4, heads)),
            dma((heads,)),
            dma((heads,)),
            dma((heads,)),
            dma((heads,)),
            dma((2, 2, n // 2)),
            dma((2, 2, n // 2)),
        ],
        compiler_params=pltpu.CompilerParams(
            collective_id=0, has_side_effects=True, vmem_limit_bytes=60 * 2**20
        ),
        name="contrastive",
    )(
        pic,
        split,
        cap,
        gain.reshape(1, width),
        gain.reshape(heads, 1, cols),
        entry,
        exit_,
        mapping,
        scale.reshape(1, 1),
        shift.reshape(1, 1),
    )
    first = lax.axis_index("mp") * cols
    grad_image = lax.dynamic_slice_in_dim(go, first, cols, 1).astype(F32) + rest
    return grad_image, text


def solution(mesh):
    in_specs = (
        P("dp", None),
        P("dp", "mp"),
        P(),
        P(None, "mp"),
        P("mp", None),
        P("mp", None),
        P(),
        P(),
    )
    out_specs = (P("dp", "mp"), P("dp", "mp"))
    return jax.shard_map(
        per_device, mesh=mesh, in_specs=in_specs, out_specs=out_specs, check_vma=False
    )
```

```python
import functools
import math

import jax
import jax.numpy as jnp
from jax import lax
from jax.experimental import pallas as pl
from jax.experimental.pallas import tpu as pltpu
from jax.sharding import PartitionSpec as P

F32 = jnp.float32
BF16 = jnp.bfloat16
MESH = pl.DeviceIdType.MESH
TILE = 512
ROOT = math.sqrt(2.0 / math.pi)
NT = (((1,), (1,)), ((), ()))


def dot(a, b):
    return jnp.dot(a, b, preferred_element_type=F32)


def dot_nt(a, b):
    return lax.dot_general(a, b, NT, preferred_element_type=F32)


def gelu_pair(x):
    square = x * x
    t = jnp.tanh(ROOT * (x + 0.044715 * (square * x)))
    half = 0.5 * (1.0 + t)
    slope = half + 0.5 * x * (1.0 - t * t) * (ROOT * (1.0 + 0.134145 * square))
    return x * half, slope


def norm_back(upstream, unit_rows, inverse):
    unit_float = unit_rows.astype(F32)
    along = jnp.sum(unit_float * upstream, axis=-1, keepdims=True)
    return inverse * (upstream - unit_float * along)


def body(
    n,
    heads,
    pic_hbm,
    cap_hbm,
    gain_ref,
    entry_hbm,
    exit_hbm,
    map_hbm,
    scale_ref,
    shift_ref,
    out_go,
    out_rest,
    out_text,
    pic,
    cap,
    entry,
    exit_,
    mapping,
    load_sem,
    normed,
    slope,
    acc,
    own_f32,
    parts,
    lands,
    fulls,
    ring_text,
    ring_image,
    gains,
    centres,
    norm_own,
    norm_part,
    norm_land,
    sums_part,
    sums_land,
    part_send,
    part_recv,
    full_send,
    full_recv,
    norm_send,
    norm_recv,
    sums_send,
    sums_recv,
    ring_send,
    ring_recv,
):
    rows, width = pic.shape
    share = rows // heads
    hidden = exit_.shape[0]
    cols = width // heads
    me = lax.axis_index("dp")
    head = lax.axis_index("mp")
    length = n // 4

    def place(index):
        z = index // 4
        y = (index // 2) % 2
        return 2 * (z * (1 - y) + (2 * length - 1 - z) * y) + index % 2

    def device(position):
        position = (position + n) % n
        chip = position // 2
        y = chip // length
        z = chip * (1 - y) + (2 * length - 1 - chip) * y
        return (z * 2 + y) * 2 + position % 2

    pos = place(me)
    right = device(pos + 1)
    left = device(pos - 1)
    forward = n // 2
    backward = n - 1 - forward

    loads = []
    for at, (src, dst) in enumerate(
        (
            (cap_hbm, cap),
            (map_hbm, mapping),
            (pic_hbm, pic),
            (entry_hbm, entry),
            (exit_hbm, exit_),
        )
    ):
        copy = pltpu.make_async_copy(src, dst, load_sem.at[at])
        copy.start()
        loads.append(copy)

    barrier = pltpu.get_barrier_semaphore()
    for neighbour in (left, right):
        pl.semaphore_signal(barrier, inc=1, device_id={"dp": neighbour}, device_id_type=MESH)
    for o in range(1, heads):
        pl.semaphore_signal(
            barrier, inc=1, device_id={"mp": (head + o) % heads}, device_id_type=MESH
        )

    def ring_copy(which, buf, way, step):
        block = device(pos - step if way == 0 else pos + step)
        return pltpu.make_async_remote_copy(
            src_ref=buf.at[block],
            dst_ref=buf.at[block],
            send_sem=ring_send.at[which, way, step],
            recv_sem=ring_recv.at[which, way, step],
            device_id={"dp": right if way == 0 else left},
            device_id_type=MESH,
        )

    def ring_start(which, buf, step):
        if step < forward:
            ring_copy(which, buf, 0, step).start()
        if step < backward:
            ring_copy(which, buf, 1, step).start()

    def ring_next(which, buf, step):
        for way, count in ((0, forward), (1, backward)):
            if step < count:
                block = device(pos - step - 1 if way == 0 else pos + step + 1)
                pltpu.make_async_remote_copy(
                    src_ref=buf.at[block],
                    dst_ref=buf.at[block],
                    send_sem=ring_send.at[which, way, step],
                    recv_sem=ring_recv.at[which, way, step],
                    device_id={"dp": right if way == 0 else left},
                    device_id_type=MESH,
                ).wait_recv()
                if step + 1 < count:
                    ring_copy(which, buf, way, step + 1).start()

    def ring_end(which, buf):
        for way, count in ((0, forward), (1, backward)):
            for step in range(count):
                ring_copy(which, buf, way, step).wait_send()

    def exchange(src, dst, send, recv, spread):
        copies = []
        for o in range(1, heads):
            to = (head + o) % heads
            source = (head + heads - o) % heads
            sent = pltpu.make_async_remote_copy(
                src_ref=src.at[to] if spread else src.at[head],
                dst_ref=dst.at[head],
                send_sem=send.at[o],
                recv_sem=recv.at[o],
                device_id={"mp": to},
                device_id_type=MESH,
            )
            got = pltpu.make_async_remote_copy(
                src_ref=dst.at[source],
                dst_ref=dst.at[source],
                send_sem=send.at[o],
                recv_sem=recv.at[o],
                device_id={"mp": to},
                device_id_type=MESH,
            )
            copies.append((sent, got))
        for sent, got in copies:
            sent.start()
        return copies

    def arrived(copies):
        for sent, got in copies:
            got.wait_recv()

    def finished(copies):
        for sent, got in copies:
            sent.wait_send()

    def scatter_start(which, total):
        for p in range(heads):
            piece = total[p * share : (p + 1) * share]
            own_f32[p] = piece
            parts[which, p] = piece.astype(BF16)
        return exchange(
            parts.at[which], lands.at[which], part_send.at[which], part_recv.at[which], True
        )

    def scatter_sum(which, copies, mine):
        arrived(copies)
        for o in range(1, heads):
            mine = mine + lands[which, (head + heads - o) % heads].astype(F32)
        return mine

    def share_start(which, mine):
        fulls[which, head] = mine
        return exchange(
            fulls.at[which], fulls.at[which], full_send.at[which], full_recv.at[which], False
        )

    def full(which):
        return jnp.concatenate([fulls[which, p] for p in range(heads)], axis=0)

    pending = []

    loads[0].wait()
    loads[1].wait()
    text_part = dot(cap[...], mapping[...])
    pl.semaphore_wait(barrier, 2 + heads - 1)
    text_copies = scatter_start(0, text_part)
    pending.append(text_copies)
    text_mine = own_f32[head]

    loads[2].wait()
    image_float = pic[...].astype(F32)
    mean_row = jnp.mean(image_float, axis=-1, keepdims=True)
    variance = jnp.mean((image_float - mean_row) ** 2, axis=-1, keepdims=True)
    inv_std = lax.rsqrt(variance + 1e-06)
    gain = gain_ref[...].reshape(1, width)
    centred = (image_float - mean_row) * inv_std
    normed[...] = (centred * gain).astype(BF16)
    for p in range(heads):
        gains[p] = gain[:, p * cols : (p + 1) * cols]
        centres[p] = centred[:, p * cols : (p + 1) * cols]

    text_out = scatter_sum(0, text_copies, text_mine)
    inv_text = lax.rsqrt(jnp.sum(text_out * text_out, axis=-1, keepdims=True) + 1e-06)
    unit_text = (text_out * inv_text).astype(BF16)
    ring_text[me] = unit_text
    ring_start(0, ring_text, 0)
    text_full = share_start(0, unit_text)
    pending.append(text_full)

    loads[3].wait()
    loads[4].wait()
    tiles = [(first, min(TILE, hidden - first)) for first in range(0, hidden, TILE)]
    text_steps = iter(range(forward))

    def advance(steps, which, buf, count):
        for _ in range(count):
            step = next(steps, None)
            if step is not None:
                ring_next(which, buf, step)

    for at, (first, size) in enumerate(tiles):
        span = slice(first, first + size)
        value, grad = gelu_pair(dot_nt(normed[...], entry[span, :]))
        slope[:, span] = grad
        product = dot(value.astype(BF16), exit_[span, :])
        if at == 0:
            acc[...] = product
        else:
            acc[...] += product
        if at % 2 == 1:
            advance(text_steps, 0, ring_text, 1)
    image_copies = scatter_start(1, acc[...])
    pending.append(image_copies)
    mine = own_f32[head] + pic[pl.ds(pl.multiple_of(head * share, 8), share), :].astype(F32)
    advance(text_steps, 0, ring_text, 2)
    image_out = scatter_sum(1, image_copies, mine)
    inv_image = lax.rsqrt(jnp.sum(image_out * image_out, axis=-1, keepdims=True) + 1e-06)
    unit_image = (image_out * inv_image).astype(BF16)
    ring_image[me] = unit_image
    image_full = share_start(1, unit_image)
    pending.append(image_full)
    ring_start(1, ring_image, 0)
    advance(text_steps, 0, ring_text, forward)
    ring_end(0, ring_text)
    arrived(image_full)
    arrived(text_full)

    scale = scale_ref[0, 0]
    shift = shift_ref[0, 0]
    group = 4 if share % 16 == 0 else 1

    def terms(rows_ref, buf):
        acc[...] = jnp.zeros_like(acc)

        def one(g, carry):
            mine = full(rows_ref)
            if group == 1:
                block = buf[g]
            else:
                block = buf[pl.ds(g * group, group)].reshape(group * share, width)
            energy = scale * dot_nt(mine, block) + shift
            shape = (rows, group * share)
            column = lax.broadcasted_iota(jnp.int32, shape, 1)
            ident = column + (g * (group * rows) + head * share)
            for j in range(1, group):
                ident = ident + jnp.where(column >= j * share, rows - share, 0)
            same = ident == lax.broadcasted_iota(jnp.int32, shape, 0) + me * rows
            weight = scale * jax.nn.sigmoid(jnp.where(same, -energy, energy))
            weight = jnp.where(same, -weight, weight).astype(BF16)
            acc[...] += dot(weight, block)
            return carry

        lax.fori_loop(0, n // group, one, 0)

    image_steps = iter(range(forward))
    terms(1, ring_text)
    dir_copies = scatter_start(2, acc[...])
    pending.append(dir_copies)
    dir_mine = own_f32[head]
    advance(image_steps, 1, ring_image, 4)
    image_dir = scatter_sum(2, dir_copies, dir_mine)
    grad_out = norm_back(image_dir, fulls[1, head], inv_image)
    grad_full = share_start(2, grad_out.astype(BF16))
    pending.append(grad_full)
    advance(image_steps, 1, ring_image, forward)
    ring_end(1, ring_image)

    terms(0, ring_image)
    dirs_copies = scatter_start(3, acc[...])
    pending.append(dirs_copies)
    dirs_mine = own_f32[head]

    arrived(grad_full)
    for p in range(heads):
        out_go[p * share : (p + 1) * share] = fulls[2, p]
    grad_b = full(2)
    for at, (first, size) in enumerate(tiles):
        span = slice(first, first + size)
        grad_pre = (dot_nt(grad_b, exit_[span, :]) * slope[:, span]).astype(BF16)
        product = dot(grad_pre, entry[span, :])
        if at == 0:
            acc[...] = product
        else:
            acc[...] += product
    total = acc[...]
    for p in range(heads):
        piece = total[:, p * cols : (p + 1) * cols]
        norm_own[p] = piece
        norm_part[p] = piece.astype(BF16)
    norm_copies = exchange(norm_part, norm_land, norm_send, norm_recv, True)
    scaled = total * gain_ref[...].reshape(1, width)
    one_sum = jnp.sum(scaled, axis=-1, keepdims=True)
    centred = (pic[...].astype(F32) - mean_row) * inv_std
    two_sum = jnp.sum(scaled * centred, axis=-1, keepdims=True)
    lane = lax.broadcasted_iota(jnp.int32, (rows, 128), 1)
    sums_part[head] = jnp.where(lane == 0, one_sum, two_sum)
    sums_copies = exchange(sums_part, sums_land, sums_send, sums_recv, False)
    pending.append(norm_copies)
    pending.append(sums_copies)

    text_dir = scatter_sum(3, dirs_copies, dirs_mine)
    grad_text_out = norm_back(text_dir, fulls[0, head], inv_text).astype(BF16)
    last_full = share_start(3, grad_text_out)
    pending.append(last_full)

    arrived(norm_copies)
    arrived(sums_copies)
    grad_normed = norm_own[head]
    sums = sums_part[head]
    for o in range(1, heads):
        source = (head + heads - o) % heads
        grad_normed = grad_normed + norm_land[source].astype(F32)
        sums = sums + sums_land[source]
    mean_one = sums[:, 0:1] * (1.0 / width)
    mean_two = sums[:, 1:2] * (1.0 / width)
    centred = centres[head]
    scaled = grad_normed * gains[head]
    out_rest[...] = inv_std * (scaled - mean_one - centred * mean_two)

    arrived(last_full)
    out_text[...] = dot_nt(full(3), mapping[...])
    for copies in pending:
        finished(copies)


def per_device(pic, cap, gain, entry, exit_, mapping, scale, shift):
    rows, width = pic.shape
    n = lax.axis_size("dp")
    heads = lax.axis_size("mp")
    cols = cap.shape[1]
    share = rows // heads
    hidden = entry.shape[1]
    flipped = entry.T
    anywhere = pl.BlockSpec(memory_space=pl.ANY)
    vmem = pl.BlockSpec(memory_space=pltpu.VMEM)
    smem = pl.BlockSpec(memory_space=pltpu.SMEM)
    dma = pltpu.SemaphoreType.DMA
    go, rest, text = pl.pallas_call(
        functools.partial(body, n, heads),
        out_shape=(
            jax.ShapeDtypeStruct((rows, width), BF16),
            jax.ShapeDtypeStruct((rows, cols), F32),
            jax.ShapeDtypeStruct((rows, mapping.shape[0]), F32),
        ),
        in_specs=[anywhere, anywhere, vmem, anywhere, anywhere, anywhere, smem, smem],
        out_specs=(vmem, vmem, vmem),
        scratch_shapes=[
            pltpu.VMEM(pic.shape, BF16),
            pltpu.VMEM(cap.shape, BF16),
            pltpu.VMEM(flipped.shape, BF16),
            pltpu.VMEM(exit_.shape, BF16),
            pltpu.VMEM(mapping.shape, BF16),
            dma((5,)),
            pltpu.VMEM((rows, width), BF16),
            pltpu.VMEM((rows, hidden), F32),
            pltpu.VMEM((rows, width), F32),
            pltpu.VMEM((heads, share, width), F32),
            pltpu.VMEM((4, heads, share, width), BF16),
            pltpu.VMEM((4, heads, share, width), BF16),
            pltpu.VMEM((4, heads, share, width), BF16),
            pltpu.VMEM((n, share, width), BF16),
            pltpu.VMEM((n, share, width), BF16),
            pltpu.VMEM((heads, 1, cols), F32),
            pltpu.VMEM((heads, rows, cols), F32),
            pltpu.VMEM((heads, rows, cols), F32),
            pltpu.VMEM((heads, rows, cols), BF16),
            pltpu.VMEM((heads, rows, cols), BF16),
            pltpu.VMEM((heads, rows, 128), F32),
            pltpu.VMEM((heads, rows, 128), F32),
            dma((4, heads)),
            dma((4, heads)),
            dma((4, heads)),
            dma((4, heads)),
            dma((heads,)),
            dma((heads,)),
            dma((heads,)),
            dma((heads,)),
            dma((2, 2, n // 2)),
            dma((2, 2, n // 2)),
        ],
        compiler_params=pltpu.CompilerParams(
            collective_id=0, has_side_effects=True, vmem_limit_bytes=60 * 2**20
        ),
        name="contrastive",
    )(
        pic,
        cap,
        gain,
        flipped,
        exit_,
        mapping,
        scale.reshape(1, 1),
        shift.reshape(1, 1),
    )
    first = lax.axis_index("mp") * cols
    grad_image = lax.dynamic_slice_in_dim(go, first, cols, 1).astype(F32) + rest
    return grad_image, text


def solution(mesh):
    in_specs = (
        P("dp", None),
        P("dp", "mp"),
        P(),
        P(None, "mp"),
        P("mp", None),
        P("mp", None),
        P(),
        P(),
    )
    out_specs = (P("dp", "mp"), P("dp", "mp"))
    return jax.shard_map(
        per_device, mesh=mesh, in_specs=in_specs, out_specs=out_specs, check_vma=False
    )
```
